256 devices in a mesh: freq: 8 (over x, core), rec: 32 (over z, y).
Axes of the slice: x: 4, y: 4, z: 8, core: 2. Of those that a mesh axis runs over, the one named last changes fastest.
Arguments:
- response_real: float32 [96, 1536, 1536], P('freq', 'rec'), may hold values from -0.109375 to 0.109375
- response_imaginary: float32 [96, 1536, 1536], P('freq', 'rec'), may hold values from -0.109375 to 0.109375
- focus: float32 [1536, 96, 128], P('rec', 'freq'), may hold values from -6 to 6
- initial: float32 [1536, 96, 128], P('rec', 'freq'), may hold values from -6 to 6
- onset: int32 [1536, 64], P('rec'), may hold values from 24 to 167
Outputs:
- focus_next: float32 [1536, 96, 128], P('rec', 'freq')
The draws below stay inside these ranges and needn't reach their ends.
All inputs are finite; a program needn't handle non-finite values.
Results may differ from the reference program's by a relative error of at most 0.0003.
Values sent between devices are 32-bit elements; how exact they have to be, the bound alone decides.
No kernel may reach another device: no remote copies, remote signals or barrier semaphores. Data moves between devices by JAX's collectives and lax.ppermute only.
A program may use at most 128 MiB of HBM per device.

```python
import math
import jax
import jax.numpy as jnp
from jax import lax

F = 96
NPOS = 1536
P_SIZE = 64
NT = 192


def set_ends(drawn, own_key, least, top_value):
    dims = drawn.shape
    place = [jax.random.randint(jax.random.fold_in(own_key, axis), (), 0, dims[axis]) for axis in range(len(dims))]
    drawn = drawn.at[tuple(place)].set(least)
    longest = dims.index(max(dims))
    place[longest] = (place[longest] + 1) % dims[longest]
    return drawn.at[tuple(place)].set(top_value)


def shard_levels(stream_key, shape, pieces, smallest, top_value):
    factor_of = 1.0
    for axis_at, blocks in pieces:
        steps = jax.random.uniform(jax.random.fold_in(jax.random.fold_in(stream_key, 6), axis_at), (blocks,), jnp.float32, smallest / len(pieces), top_value / len(pieces))
        factor_of = factor_of * jnp.repeat(jnp.exp(steps), shape[axis_at] // blocks).reshape((-1,) + (1,) * (len(shape) - 1 - axis_at))
    return factor_of


def scatter_about(stream_key, dims, spread, most, cuts=(), held_as=jnp.bfloat16):
    level = shard_levels(stream_key, dims, cuts, -0.22, 0.18) if cuts else 1.0
    values = jax.random.normal(stream_key, dims, jnp.float32) * spread * level
    return jnp.minimum(jnp.maximum(values, -most), most).astype(held_as)


def setup_inputs(seed: int = 0) -> dict:
    key_of = jax.random.split(jax.random.key(seed), 6)
    return {
        "response_real": scatter_about(key_of[0], (F, NPOS, NPOS), (2 * NPOS) ** -0.5, 0.109375, ((0, 8), (1, 32)), jnp.float32),
        "response_imaginary": scatter_about(key_of[1], (F, NPOS, NPOS), (2 * NPOS) ** -0.5, 0.109375, ((0, 8), (1, 32)), jnp.float32),
        "focus": scatter_about(key_of[2], (NPOS, F, 2 * P_SIZE), 1.0, 6.0, ((0, 32), (1, 8)), jnp.float32),
        "initial": scatter_about(key_of[3], (NPOS, F, 2 * P_SIZE), 1.0, 6.0, ((0, 32), (1, 8)), jnp.float32),
        "onset": set_ends(jax.random.randint(key_of[4], (NPOS, P_SIZE), NT // 8, NT - NT // 8), jax.random.fold_in(key_of[4], 1), NT // 8, (NT - NT // 8) - 1).astype(jnp.int32),
    }


def tables(freqs):
    samples = 2 * freqs
    order = lax.iota(jnp.int32, freqs)
    sample = lax.iota(jnp.int32, samples)
    phase = (order[:, None] * sample[None, :]) % samples
    phases = (2.0 * math.pi / samples) * phase.astype(jnp.float32)
    cosine = jnp.cos(phases)
    sine = jnp.sin(phases)
    factor = jnp.where(order == 0, 1.0, 2.0).astype(jnp.float32)[:, None] / samples
    inverse = jnp.stack([factor * cosine, -factor * sine])
    forward = jnp.stack([cosine, -sine])
    return inverse, forward, sample


def window(spectrum, onset):
    count, freqs, width = spectrum.shape
    half = width // 2
    inverse, forward, sample = tables(freqs)
    split = spectrum.reshape(count, freqs, 2, half)
    traces = jnp.einsum("nkcp,ckt->ntp", split, inverse, precision=lax.Precision.HIGHEST)
    keep = sample[None, :, None] < onset[:, None, :]
    clipped = jnp.where(keep, traces, 0.0)
    back = jnp.einsum("ntp,ckt->nkcp", clipped, forward, precision=lax.Precision.HIGHEST)
    return back.reshape(count, freqs, width)


def adjoint_terms(real_part, imag_part, values):
    half = values.shape[2] // 2
    first = jnp.einsum("frs,rfq->sfq", real_part, values, precision=lax.Precision.HIGHEST)
    second = jnp.einsum("frs,rfq->sfq", imag_part, values, precision=lax.Precision.HIGHEST)
    return jnp.concatenate([first[..., :half] + second[..., half:], first[..., half:] - second[..., :half]], axis=2)


def forward_terms(real_part, imag_part, values):
    half = values.shape[2] // 2
    first = jnp.einsum("frs,sfq->rfq", real_part, values, precision=lax.Precision.HIGHEST)
    second = jnp.einsum("frs,sfq->rfq", imag_part, values, precision=lax.Precision.HIGHEST)
    return jnp.concatenate([first[..., :half] - second[..., half:], first[..., half:] + second[..., :half]], axis=2)


def reference(response_real, response_imaginary, focus, initial, onset):
    adjoint = adjoint_terms(response_real, response_imaginary, focus)
    windowed = window(adjoint, onset)
    forward = forward_terms(response_real, response_imaginary, windowed)
    return initial - window(forward, onset)
```

```python
import math

import jax
import jax.numpy as jnp
import numpy as np
from jax import lax
from jax.experimental import pallas as pl
from jax.experimental.pallas import tpu as pltpu
from jax.sharding import Mesh
from jax.sharding import PartitionSpec as P

REC = ("z", "y")
Z_FIRST = 5
INTERPRET = False
KERNEL_VMEM = 16 << 20
CUTS_Z = 1
CUTS_Y = 2


def split(x):
    high = x.astype(jnp.bfloat16)
    low = (x - high.astype(jnp.float32)).astype(jnp.bfloat16)
    return high, low


def swap_halves(x):
    return pltpu.roll(x, x.shape[-1] // 2, x.ndim - 1)


def left_half(shape):
    return lax.broadcasted_iota(jnp.int32, shape, len(shape) - 1) < shape[-1] // 2


def block_row(place, up, across, outer, inner):
    return lax.rem(place[0] + up, outer) * inner + lax.rem(place[1] + across, inner)


def adjoint_blocks(place, real_part, imag_part, values, first, count, by_inner, cuts, outer, inner):
    _, rows, sources = real_part.shape
    width = values.shape[2]
    block = sources // (outer * inner)
    part = block // cuts
    leading, trailing = (inner, outer) if by_inner else (outer, inner)

    def kernel(place, real_ref, imag_ref, values_ref, *refs):
        rows_ref = refs[-1]
        values = values_ref[0]
        swapped = swap_halves(values)
        swapped = jnp.where(left_half(values.shape), swapped, -swapped)
        v_high, v_low = split(jnp.concatenate([values, swapped], axis=0))
        r_high, r_low = split(jnp.concatenate([real_ref[0], imag_ref[0]], axis=0))
        side = jnp.concatenate([v_high, v_low], axis=1)
        both = jnp.concatenate([side, side], axis=0)
        stacked = jnp.concatenate([r_high, r_low], axis=0)
        product = lax.dot_general(
            stacked, both, (((0,), (0,)), ((), ())), preferred_element_type=jnp.float32
        )
        rows_ref[...] = product[:, :width] + product[:, width:]
        for i in range(leading):
            for j in range(trailing):
                up, across = (j, i) if by_inner else (i, j)
                at = block_row(place, up, across, outer, inner) * block
                for cut in range(cuts):
                    refs[cuts * i + cut][j, 0] = rows_ref[pl.ds(pl.multiple_of(at + cut * part, 8), part), :]

    shape = jax.ShapeDtypeStruct((trailing, count, part, width), jnp.float32)
    found = pl.pallas_call(
        kernel,
        grid_spec=pltpu.PrefetchScalarGridSpec(
            num_scalar_prefetch=1,
            grid=(count,),
            in_specs=[
                pl.BlockSpec((1, rows, sources), lambda f, place: (f + first, 0, 0)),
                pl.BlockSpec((1, rows, sources), lambda f, place: (f + first, 0, 0)),
                pl.BlockSpec((1, rows, width), lambda f, place: (f + first, 0, 0)),
            ],
            out_specs=[pl.BlockSpec((trailing, 1, part, width), lambda f, place: (0, f, 0, 0))] * (cuts * leading),
            scratch_shapes=[pltpu.VMEM((sources, width), jnp.float32)],
        ),
        out_shape=[shape] * (cuts * leading),
        compiler_params=pltpu.CompilerParams(vmem_limit_bytes=KERNEL_VMEM),
        interpret=INTERPRET,
        name="adjoint_y" if by_inner else "adjoint_z",
    )(place, real_part, imag_part, values)
    return [found[cuts * i : cuts * i + cuts] for i in range(leading)]


def forward_blocks(place, real_part, imag_part, order, pieces, first, count, by_inner, outer, inner):
    _, rows, sources = real_part.shape
    width = pieces[0][2].shape[-1]
    block = sources // (outer * inner)

    def kernel(place, real_ref, imag_ref, *refs):
        parts, out_ref, rows_ref = refs[:-2], refs[-2], refs[-1]
        for (second, row, _), held in zip(pieces, parts):
            for j, offset in enumerate(order):
                up, across = (offset, second) if by_inner else (second, offset)
                at = block_row(place, up, across, outer, inner) * block + row
                rows_ref[pl.ds(pl.multiple_of(at, 8), held.shape[2]), :] = held[j, 0]
        v_high, v_low = split(rows_ref[...])
        r_high, r_low = split(jnp.concatenate([real_ref[0], imag_ref[0]], axis=0))
        product = jnp.dot(
            jnp.concatenate([r_high, r_low], axis=0),
            jnp.concatenate([v_high, v_low], axis=1),
            preferred_element_type=jnp.float32,
        )
        total = product[: 2 * rows] + product[2 * rows :]
        total = total[:, :width] + total[:, width:]
        crossed = swap_halves(total[rows:])
        out_ref[0] = total[:rows] + jnp.where(left_half(crossed.shape), -crossed, crossed)

    return pl.pallas_call(
        kernel,
        grid_spec=pltpu.PrefetchScalarGridSpec(
            num_scalar_prefetch=1,
            grid=(count,),
            in_specs=[
                pl.BlockSpec((1, rows, sources), lambda f, place: (f + first, 0, 0)),
                pl.BlockSpec((1, rows, sources), lambda f, place: (f + first, 0, 0)),
            ]
            + [
                pl.BlockSpec((len(order), 1) + piece.shape[2:], lambda f, place: (0, f, 0, 0))
                for _, _, piece in pieces
            ],
            out_specs=pl.BlockSpec((1, rows, width), lambda f, place: (f, 0, 0)),
            scratch_shapes=[pltpu.VMEM((sources, width), jnp.float32)],
        ),
        out_shape=jax.ShapeDtypeStruct((count, rows, width), jnp.float32),
        compiler_params=pltpu.CompilerParams(vmem_limit_bytes=KERNEL_VMEM),
        interpret=INTERPRET,
        name="forward_y" if by_inner else "forward_z",
    )(place, real_part, imag_part, *[piece for _, _, piece in pieces])


def tables(freqs):
    samples = 2 * freqs
    phase = np.arange(freqs)[:, None] * np.arange(samples)[None, :] % samples
    angle = 2.0 * math.pi / samples * phase
    factor = np.where(np.arange(freqs) == 0, 1.0, 2.0)[:, None] / samples
    inverse = np.concatenate([factor * np.cos(angle), -factor * np.sin(angle)]).T
    forward = np.concatenate([np.cos(angle), -np.sin(angle)])
    return np.asarray(inverse, np.float32), np.asarray(forward, np.float32)


def window_kernel(inverse_ref, forward_ref, onset_ref, x_ref, out_ref):
    freqs, count, width = x_ref.shape
    left = left_half((freqs, width))
    columns = []
    for n in range(count):
        x = x_ref[:, n, :]
        turned = swap_halves(x)
        columns.append(jnp.concatenate([jnp.where(left, x, turned), jnp.where(left, turned, x)], axis=0))
    spectrum = jnp.concatenate(columns, axis=1)
    traces = jnp.dot(
        inverse_ref[...], spectrum, precision=lax.Precision.HIGHEST, preferred_element_type=jnp.float32
    )
    onset = jnp.concatenate([onset_ref[n : n + 1, :] for n in range(count)], axis=1)
    sample = lax.broadcasted_iota(jnp.int32, traces.shape, 0)
    clipped = jnp.where(sample < onset, traces, 0.0)
    back = jnp.dot(
        forward_ref[...], clipped, precision=lax.Precision.HIGHEST, preferred_element_type=jnp.float32
    )
    for n in range(count):
        one = back[:, n * width : (n + 1) * width]
        out_ref[:, n, :] = jnp.where(left, one[:freqs], one[freqs:])


def window(x, onset):
    inverse, forward = tables(x.shape[0])
    return pl.pallas_call(
        window_kernel,
        out_shape=jax.ShapeDtypeStruct(x.shape, jnp.float32),
        compiler_params=pltpu.CompilerParams(vmem_limit_bytes=KERNEL_VMEM),
        interpret=INTERPRET,
        name="window",
    )(jnp.asarray(inverse), jnp.asarray(forward), onset, x)


def shift(x, axis, step):
    size = lax.axis_size(axis)
    return lax.ppermute(x, axis, [(i, (i + step) % size) for i in range(size)])


def reaches(size, cuts):
    far, near = size // 2, size - 1 - size // 2
    return ((far, near), (near, far))[:cuts]


def ring_sum(blocks, axis):
    size = lax.axis_size(axis)
    cuts = len(blocks[0])
    moved = {}
    for d in range(size // 2, 0, -1):
        for cut, reach in enumerate(reaches(size, cuts)):
            for sign, steps in zip((1, -1), reach):
                if d <= steps:
                    mine = blocks[sign * d % size][cut]
                    held = moved.get((cut, sign))
                    moved[cut, sign] = shift(mine if held is None else mine + held, axis, sign)
    return [blocks[0][cut] + moved[cut, 1] + moved[cut, -1] for cut in range(cuts)]


def ring_share(cuts, axis):
    size = lax.axis_size(axis)
    found = [(0, cut, x) for cut, x in enumerate(cuts)]
    moved = {}
    for d in range(1, size // 2 + 1):
        for cut, reach in enumerate(reaches(size, len(cuts))):
            for sign, steps in zip((1, -1), reach):
                if d <= steps:
                    moved[cut, sign] = shift(moved.get((cut, sign), cuts[cut]), axis, sign)
                    found.append((-sign * d % size, cut, moved[cut, sign]))
    return found


def reduce_blocks(blocks, first_axis, second_axis):
    cuts = ring_sum(blocks, first_axis)
    size = lax.axis_size(second_axis)
    whole = [[jnp.concatenate([cut[d] for cut in cuts], axis=1)] for d in range(size)]
    return ring_sum(whole, second_axis)[0]


def share_blocks(block, first_axis, second_axis, cuts):
    found = ring_share([block], first_axis)
    part = block.shape[1] // cuts
    whole = [jnp.stack([x[:, cut * part : (cut + 1) * part] for _, _, x in found]) for cut in range(cuts)]
    pieces = [(offset, cut * part, x) for offset, cut, x in ring_share(whole, second_axis)]
    return [offset for offset, _, _ in found], pieces


def on_device(response_real, response_imaginary, focus, initial, onset):
    values = focus.transpose(1, 0, 2)
    freqs = values.shape[0]
    z_first = Z_FIRST * freqs // 12
    place = jnp.stack([lax.axis_index("z"), lax.axis_index("y")]).astype(jnp.int32)
    owned = onset.shape[0] // lax.axis_size("freq")
    local = lax.dynamic_slice_in_dim(onset, lax.axis_index("freq") * owned, owned, 0)
    local = jnp.concatenate([local, local], axis=1)
    outer, inner = lax.axis_size("z"), lax.axis_size("y")

    def turn(x):
        return lax.all_to_all(x, "freq", split_axis=1, concat_axis=0, tiled=True)

    def turn_back(x):
        return lax.all_to_all(x, "freq", split_axis=0, concat_axis=1, tiled=True)

    blocks_y = adjoint_blocks(
        place, response_real, response_imaginary, values, z_first, freqs - z_first, True, CUTS_Y, outer, inner
    )
    blocks_z = adjoint_blocks(
        place, response_real, response_imaginary, values, 0, z_first, False, CUTS_Z, outer, inner
    )
    sum_y = reduce_blocks(blocks_y, "y", "z")
    sum_z = reduce_blocks(blocks_z, "z", "y")
    adjoint = jnp.concatenate([sum_z, sum_y], axis=0)
    windowed = turn_back(window(turn(adjoint), local))
    pieces_y = share_blocks(windowed[z_first:], "z", "y", CUTS_Y)
    pieces_z = share_blocks(windowed[:z_first], "y", "z", CUTS_Z)
    forward_z = forward_blocks(
        place, response_real, response_imaginary, *pieces_z, 0, z_first, False, outer, inner
    )
    forward_y = forward_blocks(
        place, response_real, response_imaginary, *pieces_y, z_first, freqs - z_first, True, outer, inner
    )
    forward = jnp.concatenate([forward_z, forward_y], axis=0)
    update = turn_back(window(turn(forward), local))
    return initial - update.transpose(1, 0, 2)


def solution(mesh):
    finer = Mesh(mesh.devices.reshape(mesh.shape["freq"], 8, 4), ("freq", "z", "y"))
    in_specs = (
        P("freq", REC, None),
        P("freq", REC, None),
        P(REC, "freq", None),
        P(REC, "freq", None),
        P(REC, None),
    )
    out_specs = P(REC, "freq", None)
    return jax.shard_map(
        on_device, mesh=finer, in_specs=in_specs, out_specs=out_specs, check_vma=False
    )
```

```python
import math

import jax
import jax.numpy as jnp
import numpy as np
from jax import lax
from jax.experimental import pallas as pl
from jax.experimental.pallas import tpu as pltpu
from jax.sharding import Mesh
from jax.sharding import PartitionSpec as P


REC = ("z", "y")
CHUNKS = (2, 1)
TILE = 8
KERNEL_VMEM = 24 << 20


def split(x):
    high = x.astype(jnp.bfloat16)
    low = (x - high.astype(jnp.float32)).astype(jnp.bfloat16)
    return high, low


def swap_halves(x):
    return pltpu.roll(x, x.shape[-1] // 2, x.ndim - 1)


def left_half(shape):
    return lax.broadcasted_iota(jnp.int32, shape, len(shape) - 1) < shape[-1] // 2


def limits():
    return pltpu.CompilerParams(vmem_limit_bytes=KERNEL_VMEM)


def adjoint_rows(reals, imags, values):
    parts, sides = [], []
    for real, imag, value in zip(reals, imags, values):
        swapped = swap_halves(value)
        parts += [real, imag]
        sides += [value, jnp.where(left_half(value.shape), swapped, -swapped)]
    r_high, r_low = split(jnp.concatenate(parts, axis=0))
    v_high, v_low = split(jnp.concatenate(sides, axis=0))
    side = jnp.concatenate([v_high, v_low], axis=1)
    product = lax.dot_general(
        jnp.concatenate([r_high, r_low], axis=0),
        jnp.concatenate([side, side], axis=0),
        (((0,), (0,)), ((), ())),
        preferred_element_type=jnp.float32,
    )
    width = values[0].shape[1]
    return product[:, :width] + product[:, width:]


def forward_rows(reals, imags, gathered):
    parts = []
    for real, imag in zip(reals, imags):
        parts += [real, imag]
    r_high, r_low = split(jnp.concatenate(parts, axis=0))
    v_high, v_low = split(gathered)
    product = jnp.dot(
        jnp.concatenate([r_high, r_low], axis=0),
        jnp.concatenate([v_high, v_low], axis=1),
        preferred_element_type=jnp.float32,
    )
    rows, width = r_high.shape[0], gathered.shape[1]
    total = product[:rows] + product[rows:]
    total = total[:, :width] + total[:, width:]
    rows = reals[0].shape[0]
    found = []
    for i in range(len(reals)):
        first, second = total[2 * i * rows : (2 * i + 1) * rows], total[(2 * i + 1) * rows : (2 * i + 2) * rows]
        crossed = swap_halves(second)
        found.append(first + jnp.where(left_half(crossed.shape), -crossed, crossed))
    return found


class Share:
    def __init__(self, count, own, up, down, far_real, far_imag):
        self.count = count
        self.arrays = [own, up, down, far_real, far_imag]
        self.rows, self.sources = far_imag.shape[1:]

    def specs(self):
        return [pl.BlockSpec((1,) + x.shape[1:], lambda f, place: (f, 0, 0)) for x in self.arrays]

    def read(self, refs):
        n = self.sources
        reals = [ref[0, :, :n] for ref in refs[:4]]
        imags = [ref[0, :, n : 2 * n] for ref in refs[:3]] + [refs[4][0]]
        values = [ref[0, :, 2 * n :] for ref in refs[:3]] + [refs[3][0, :, n:]]
        return reals, imags, values


def adjoint_blocks(place, share, width, size):
    block = share.sources // size

    def kernel(place, *refs):
        outs, rows_ref = refs[5:-1], refs[-1]
        rows_ref[...] = adjoint_rows(*share.read(refs[:5]))
        for d in range(size):
            at = lax.rem(place[0] + d, size) * block
            for tile in range(block // TILE):
                outs[d][tile, 0] = rows_ref[pl.ds(pl.multiple_of(at + tile * TILE, TILE), TILE), :]

    shape = jax.ShapeDtypeStruct((block // TILE, share.count, TILE, width), jnp.float32)
    return pl.pallas_call(
        kernel,
        grid_spec=pltpu.PrefetchScalarGridSpec(
            num_scalar_prefetch=1,
            grid=(share.count,),
            in_specs=share.specs(),
            out_specs=[pl.BlockSpec((block // TILE, 1, TILE, width), lambda f, place: (0, f, 0, 0))] * size,
            scratch_shapes=[pltpu.VMEM((share.sources, width), jnp.float32)],
        ),
        out_shape=[shape] * size,
        compiler_params=limits(),
        name="adjoint",
    )(place, *share.arrays)


def forward_blocks(place, share, pieces, first, size, fold, groups):
    width = pieces[0][2].shape[3]
    block = share.sources // size
    used = share.rows // TILE

    def kernel(place, *refs):
        out_ref, rows_ref = refs[-2], refs[-1]
        for (offset, start, _), held in zip(pieces, refs[5:-2]):
            at = lax.rem(place[0] + offset, size) * block
            for tile in range(held.shape[0]):
                row = at + (start + tile) * TILE
                rows_ref[pl.ds(pl.multiple_of(row, TILE), TILE), :] = held[tile, 0]
        reals, imags, _ = share.read(refs[:5])
        for offset, rows in zip((0, fold - 1, 1, 2), forward_rows(reals, imags, rows_ref[...])):
            at = lax.rem(place[1] + offset, fold) * groups
            for tile in range(groups):
                if tile < used:
                    out_ref[at + tile, 0] = rows[tile * TILE : (tile + 1) * TILE]
                else:
                    out_ref[at + tile, 0] = jnp.zeros((TILE, width), jnp.float32)

    return pl.pallas_call(
        kernel,
        grid_spec=pltpu.PrefetchScalarGridSpec(
            num_scalar_prefetch=1,
            grid=(share.count,),
            in_specs=share.specs()
            + [
                pl.BlockSpec((x.shape[0], 1) + x.shape[2:], lambda f, place: (0, f + first, 0, 0))
                for _, _, x in pieces
            ],
            out_specs=pl.BlockSpec((fold * groups, 1, TILE, width), lambda f, place: (0, f, 0, 0)),
            scratch_shapes=[pltpu.VMEM((share.sources, width), jnp.float32)],
        ),
        out_shape=jax.ShapeDtypeStruct((fold * groups, share.count, TILE, width), jnp.float32),
        compiler_params=limits(),
        name="forward",
    )(place, *share.arrays, *[x for _, _, x in pieces])


def tables(freqs, taken, given):
    samples = 2 * freqs
    phase = np.arange(freqs)[:, None] * np.arange(samples)[None, :] % samples
    angle = 2.0 * math.pi / samples * phase
    factor = np.where(np.arange(freqs) == 0, 1.0, 2.0)[:, None] / samples
    cosine, sine = np.cos(angle), np.sin(angle)
    inverse = np.concatenate([(factor * cosine)[taken], (-factor * sine)[taken]]).T
    forward = np.concatenate([cosine[given], -sine[given]])
    return np.asarray(inverse, np.float32), np.asarray(forward, np.float32)


def window_kernel(inverse_ref, forward_ref, onset_ref, x_ref, out_ref):
    taken, count, width = x_ref.shape
    given = out_ref.shape[0]
    left = left_half((taken, width))
    columns = []
    for n in range(count):
        x = x_ref[:, n, :]
        turned = swap_halves(x)
        columns.append(jnp.concatenate([jnp.where(left, x, turned), jnp.where(left, turned, x)], axis=0))
    spectrum = jnp.concatenate(columns, axis=1)
    traces = jnp.dot(
        inverse_ref[...], spectrum, precision=lax.Precision.HIGHEST, preferred_element_type=jnp.float32
    )
    onset = jnp.concatenate([onset_ref[n : n + 1, :] for n in range(count)], axis=1)
    sample = lax.broadcasted_iota(jnp.int32, traces.shape, 0)
    clipped = jnp.where(sample < onset, traces, 0.0)
    back = jnp.dot(
        forward_ref[...], clipped, precision=lax.Precision.HIGHEST, preferred_element_type=jnp.float32
    )
    left = left_half((given, width))
    for n in range(count):
        one = back[:, n * width : (n + 1) * width]
        out_ref[:, n, :] = jnp.where(left, one[:given], one[given:])


def window(x, onset, freqs, taken, given):
    inverse, forward = tables(freqs, taken, given)
    return pl.pallas_call(
        window_kernel,
        out_shape=jax.ShapeDtypeStruct((len(given),) + x.shape[1:], jnp.float32),
        compiler_params=limits(),
        name="window",
    )(jnp.asarray(inverse), jnp.asarray(forward), onset, x)


def shift(x, axis, step):
    size = lax.axis_size(axis)
    return lax.ppermute(x, axis, [(i, (i + step) % size) for i in range(size)])


def reaches(size, cuts):
    far, near = size // 2, size - 1 - size // 2
    return ((far, near), (near, far))[:cuts]


def ring_sum(blocks, axis, later):
    below = shift(blocks[5], axis, -1)
    moved = shift(jnp.stack([blocks[4], blocks[2]]), axis, 1)
    moved, below, later = lax.optimization_barrier((moved, below, later))
    below = shift(blocks[6] + below, axis, -1)
    leap = shift(blocks[3] + moved[0], axis, 2)
    below = shift(blocks[7] + below, axis, -1)
    above = shift(blocks[1] + moved[1] + leap, axis, 1)
    return blocks[0] + above + below, later


def ring_share(cuts, axis):
    size = lax.axis_size(axis)
    found = [(0, cut, x) for cut, x in enumerate(cuts)]
    moved = {}
    for d in range(1, size // 2 + 1):
        for cut, reach in enumerate(reaches(size, len(cuts))):
            for sign, steps in zip((1, -1), reach):
                if d <= steps:
                    moved[cut, sign] = shift(moved.get((cut, sign), cuts[cut]), axis, sign)
                    found.append((-sign * d % size, cut, moved[cut, sign]))
    return found


def chosen(x, first, count, fold, at):
    return [lax.dynamic_slice_in_dim(x, first + fold * j + at % fold, 1, 0) for j in range(count)]


def exchange(arrays, first, count, fold, y):
    def packed(d, which):
        found = [chosen(arrays[i], first, count, fold, y + d) for i in which]
        return jnp.concatenate([jnp.concatenate(one, axis=2) for one in zip(*found)], axis=0)

    far_real = shift(packed(2, (0, 2)), "y", 1)
    far_imag = shift(packed(2, (1,)), "y", -1)
    up = shift(packed(1, (0, 1, 2)), "y", 1)
    down = shift(packed(fold - 1, (0, 1, 2)), "y", -1)
    own = packed(0, (0, 1, 2))
    far_real, far_imag = shift(far_real, "y", 1), shift(far_imag, "y", -1)
    return Share(count, own, up, down, far_real, far_imag)


def on_device(response_real, response_imaginary, focus, initial, onset):
    values = focus.transpose(1, 0, 2)
    local, receivers, width = values.shape
    size, fold, groups = lax.axis_size("z"), lax.axis_size("y"), lax.axis_size("freq")
    freqs = groups * local
    pairs = local // fold
    used = receivers // TILE
    y = lax.axis_index("y")
    place = jnp.stack([lax.axis_index("z"), y]).astype(jnp.int32)
    rows = lax.dynamic_slice_in_dim(onset, lax.axis_index("freq") * TILE, TILE, 0)
    rows = jnp.concatenate([rows, rows], axis=1)
    own = [
        group * local + fold * j + side for side in range(fold) for group in range(groups) for j in range(pairs)
    ]

    def turn(x):
        return lax.all_to_all(x, ("y", "freq"), split_axis=0, concat_axis=0, tiled=True)

    def windowed_rows(x, given):
        x = turn(x).reshape(freqs, TILE, width)
        return window(x, rows, freqs, own, given)

    shares, first = [], 0
    for count in CHUNKS:
        arrays = (response_real, response_imaginary, values)
        shares.append(exchange(arrays, first, count, fold, y))
        first += fold * count

    sums = []
    for i, share in enumerate(shares):
        later = [x.arrays for x in shares[i + 1 :]]
        blocks = adjoint_blocks(place, share, width, size)
        total, later = ring_sum(blocks, "z", later)
        for x, arrays in zip(shares[i + 1 :], later):
            x.arrays = arrays
        sums.append(total)
    adjoint = jnp.concatenate(sums, axis=1).reshape(fold, used, pairs, TILE, width)
    adjoint = jnp.pad(adjoint, ((0, 0), (0, groups - used), (0, 0), (0, 0), (0, 0)))
    windowed = windowed_rows(adjoint.reshape(fold * groups, pairs, TILE, width), own)
    windowed = turn(windowed.reshape(fold * groups, pairs, TILE, width))
    windowed = windowed.reshape(fold, groups, pairs, TILE, width)[:, :used]
    windowed = windowed.reshape(fold * used, pairs, TILE, width)
    part = fold * used // 2
    found = ring_share([windowed[:part], windowed[part:]], "z")
    pieces = [(offset, cut * part, x) for offset, cut, x in found]
    parts, done = [], 0
    for share in shares:
        parts.append(forward_blocks(place, share, pieces, done, size, fold, groups))
        done += share.count
    update = windowed_rows(jnp.concatenate(parts, axis=1), list(range(freqs)))
    update = lax.all_to_all(
        update.reshape(groups, local, TILE, width), "freq", split_axis=0, concat_axis=0, tiled=True
    )
    update = update[:used].transpose(1, 0, 2, 3).reshape(local, receivers, width)
    return initial - update.transpose(1, 0, 2)


def solution(mesh):
    finer = Mesh(mesh.devices.reshape(mesh.shape["freq"], 8, 4), ("freq", "z", "y"))
    in_specs = (
        P("freq", REC, None),
        P("freq", REC, None),
        P(REC, "freq", None),
        P(REC, "freq", None),
        P(REC, None),
    )
    out_specs = P(REC, "freq", None)
    return jax.shard_map(on_device, mesh=finer, in_specs=in_specs, out_specs=out_specs, check_vma=False)
```

```python
import math

import jax
import jax.numpy as jnp
import numpy as np
from jax import lax
from jax.experimental import pallas as pl
from jax.experimental.pallas import tpu as pltpu
from jax.sharding import Mesh
from jax.sharding import PartitionSpec as P


REC = ("z", "y")
CHUNKS = (2, 1)
TILE = 8
KERNEL_VMEM = 24 << 20


def split(x):
    high = x.astype(jnp.bfloat16)
    low = (x - high.astype(jnp.float32)).astype(jnp.bfloat16)
    return high, low


def swap_halves(x):
    return pltpu.roll(x, x.shape[-1] // 2, x.ndim - 1)


def left_half(shape):
    return lax.broadcasted_iota(jnp.int32, shape, len(shape) - 1) < shape[-1] // 2


def limits():
    return pltpu.CompilerParams(vmem_limit_bytes=KERNEL_VMEM)


def adjoint_rows(reals, imags, values):
    parts, sides = [], []
    for real, imag, value in zip(reals, imags, values):
        swapped = swap_halves(value)
        parts += [real, imag]
        sides += [value, jnp.where(left_half(value.shape), swapped, -swapped)]
    r_high, r_low = split(jnp.concatenate(parts, axis=0))
    v_high, v_low = split(jnp.concatenate(sides, axis=0))
    side = jnp.concatenate([v_high, v_low], axis=1)
    product = lax.dot_general(
        jnp.concatenate([r_high, r_low], axis=0),
        jnp.concatenate([side, side], axis=0),
        (((0,), (0,)), ((), ())),
        preferred_element_type=jnp.float32,
    )
    width = values[0].shape[1]
    return product[:, :width] + product[:, width:]


def forward_rows(reals, imags, gathered):
    parts = []
    for real, imag in zip(reals, imags):
        parts += [real, imag]
    r_high, r_low = split(jnp.concatenate(parts, axis=0))
    v_high, v_low = split(gathered)
    product = jnp.dot(
        jnp.concatenate([r_high, r_low], axis=0),
        jnp.concatenate([v_high, v_low], axis=1),
        preferred_element_type=jnp.float32,
    )
    rows, width = r_high.shape[0], gathered.shape[1]
    total = product[:rows] + product[rows:]
    total = total[:, :width] + total[:, width:]
    rows = reals[0].shape[0]
    found = []
    for i in range(len(reals)):
        first, second = total[2 * i * rows : (2 * i + 1) * rows], total[(2 * i + 1) * rows : (2 * i + 2) * rows]
        crossed = swap_halves(second)
        found.append(first + jnp.where(left_half(crossed.shape), -crossed, crossed))
    return found


class Share:
    def __init__(self, count, sources, own, up, down, far_real, far_imag):
        self.count, self.rows, self.sources = count, own.shape[1], sources
        self.arrays = [own, up, down, far_real, far_imag]

    def specs(self):
        wide = self.arrays[0].shape[2]
        return [pl.BlockSpec((1, self.rows, min(wide, x.shape[2])), lambda f, place: (f, 0, 0)) for x in self.arrays]

    def read(self, refs):
        n = self.sources
        reals = [ref[0, :, :n] for ref in refs[:4]]
        imags = [ref[0, :, n : 2 * n] for ref in refs[:3]] + [refs[4][0]]
        values = [ref[0, :, 2 * n :] for ref in refs[:3]] + [refs[3][0, :, n:]]
        return reals, imags, values


def adjoint_blocks(place, share, width, size):
    block = share.sources // size

    def kernel(place, *refs):
        outs, rows_ref = refs[5:-1], refs[-1]
        rows_ref[...] = adjoint_rows(*share.read(refs[:5]))
        for d in range(size):
            at = lax.rem(place[0] + d, size) * block
            for tile in range(block // TILE):
                outs[d][tile, 0] = rows_ref[pl.ds(pl.multiple_of(at + tile * TILE, TILE), TILE), :]

    shape = jax.ShapeDtypeStruct((block // TILE, share.count, TILE, width), jnp.float32)
    return pl.pallas_call(
        kernel,
        grid_spec=pltpu.PrefetchScalarGridSpec(
            num_scalar_prefetch=1,
            grid=(share.count,),
            in_specs=share.specs(),
            out_specs=[pl.BlockSpec((block // TILE, 1, TILE, width), lambda f, place: (0, f, 0, 0))] * size,
            scratch_shapes=[pltpu.VMEM((share.sources, width), jnp.float32)],
        ),
        out_shape=[shape] * size,
        compiler_params=limits(),
        name="adjoint",
    )(place, *share.arrays)


def forward_blocks(place, share, pieces, first, size, fold, groups):
    width = pieces[0][2].shape[3]
    block = share.sources // size
    used = share.rows // TILE

    def kernel(place, *refs):
        out_ref, rows_ref = refs[-2], refs[-1]
        for (offset, start, _), held in zip(pieces, refs[5:-2]):
            at = lax.rem(place[0] + offset, size) * block
            for tile in range(held.shape[0]):
                row = at + (start + tile) * TILE
                rows_ref[pl.ds(pl.multiple_of(row, TILE), TILE), :] = held[tile, 0]
        reals, imags, _ = share.read(refs[:5])
        for offset, rows in zip((0, fold - 1, 1, 2), forward_rows(reals, imags, rows_ref[...])):
            at = lax.rem(place[1] + offset, fold) * groups
            for tile in range(groups):
                if tile < used:
                    out_ref[at + tile, 0] = rows[tile * TILE : (tile + 1) * TILE]
                else:
                    out_ref[at + tile, 0] = jnp.zeros((TILE, width), jnp.float32)

    return pl.pallas_call(
        kernel,
        grid_spec=pltpu.PrefetchScalarGridSpec(
            num_scalar_prefetch=1,
            grid=(share.count,),
            in_specs=share.specs()
            + [
                pl.BlockSpec((x.shape[0], 1) + x.shape[2:], lambda f, place: (0, f + first, 0, 0))
                for _, _, x in pieces
            ],
            out_specs=pl.BlockSpec((fold * groups, 1, TILE, width), lambda f, place: (0, f, 0, 0)),
            scratch_shapes=[pltpu.VMEM((share.sources, width), jnp.float32)],
        ),
        out_shape=jax.ShapeDtypeStruct((fold * groups, share.count, TILE, width), jnp.float32),
        compiler_params=limits(),
        name="forward",
    )(place, *share.arrays, *[x for _, _, x in pieces])


def tables(freqs, taken, given):
    samples = 2 * freqs
    phase = np.arange(freqs)[:, None] * np.arange(samples)[None, :] % samples
    angle = 2.0 * math.pi / samples * phase
    factor = np.where(np.arange(freqs) == 0, 1.0, 2.0)[:, None] / samples
    cosine, sine = np.cos(angle), np.sin(angle)
    inverse = np.concatenate([(factor * cosine)[taken], (-factor * sine)[taken]]).T
    forward = np.concatenate([cosine[given], -sine[given]])
    return np.asarray(inverse, np.float32), np.asarray(forward, np.float32)


def window_kernel(inverse_ref, forward_ref, onset_ref, x_ref, out_ref):
    taken, count, width = x_ref.shape
    given = out_ref.shape[0]
    left = left_half((taken, width))
    columns = []
    for n in range(count):
        x = x_ref[:, n, :]
        turned = swap_halves(x)
        columns.append(jnp.concatenate([jnp.where(left, x, turned), jnp.where(left, turned, x)], axis=0))
    spectrum = jnp.concatenate(columns, axis=1)
    traces = jnp.dot(
        inverse_ref[...], spectrum, precision=lax.Precision.HIGHEST, preferred_element_type=jnp.float32
    )
    onset = jnp.concatenate([onset_ref[n : n + 1, :] for n in range(count)], axis=1)
    sample = lax.broadcasted_iota(jnp.int32, traces.shape, 0)
    clipped = jnp.where(sample < onset, traces, 0.0)
    back = jnp.dot(
        forward_ref[...], clipped, precision=lax.Precision.HIGHEST, preferred_element_type=jnp.float32
    )
    left = left_half((given, width))
    for n in range(count):
        one = back[:, n * width : (n + 1) * width]
        out_ref[:, n, :] = jnp.where(left, one[:given], one[given:])


def window(x, onset, freqs, taken, given):
    inverse, forward = tables(freqs, taken, given)
    return pl.pallas_call(
        window_kernel,
        out_shape=jax.ShapeDtypeStruct((len(given),) + x.shape[1:], jnp.float32),
        compiler_params=limits(),
        name="window",
    )(jnp.asarray(inverse), jnp.asarray(forward), onset, x)


def shift(x, axis, step):
    size = lax.axis_size(axis)
    return lax.ppermute(x, axis, [(i, (i + step) % size) for i in range(size)])


def reaches(size, cuts):
    far, near = size // 2, size - 1 - size // 2
    return ((far, near), (near, far))[:cuts]


def ring_sum(blocks, axis):
    below = shift(blocks[5], axis, -1)
    moved = shift(jnp.stack([blocks[4], blocks[2]]), axis, 1)
    below = shift(blocks[6] + below, axis, -1)
    leap = shift(blocks[3] + moved[0], axis, 2)
    below = shift(blocks[7] + below, axis, -1)
    above = shift(blocks[1] + moved[1] + leap, axis, 1)
    return blocks[0] + above + below


def ring_share(cuts, axis):
    size = lax.axis_size(axis)
    found = [(0, cut, x) for cut, x in enumerate(cuts)]
    moved = {}
    for d in range(1, size // 2 + 1):
        for cut, reach in enumerate(reaches(size, len(cuts))):
            for sign, steps in zip((1, -1), reach):
                if d <= steps:
                    moved[cut, sign] = shift(moved.get((cut, sign), cuts[cut]), axis, sign)
                    found.append((-sign * d % size, cut, moved[cut, sign]))
    return found


def packed(place, arrays, first, count, fold, parts):
    rows = arrays[0].shape[1]
    widths = [arrays[i].shape[2] for _, i in parts]

    def kernel(place, *refs):
        at = 0
        for ref, width in zip(refs[:-1], widths):
            refs[-1][0, :, at : at + width] = ref[0]
            at += width

    def member(d):
        return lambda j, place: (first + fold * j + lax.rem(place[1] + d, fold), 0, 0)

    return pl.pallas_call(
        kernel,
        grid_spec=pltpu.PrefetchScalarGridSpec(
            num_scalar_prefetch=1,
            grid=(count,),
            in_specs=[pl.BlockSpec((1, rows, width), member(d)) for (d, _), width in zip(parts, widths)],
            out_specs=pl.BlockSpec((1, rows, sum(widths)), lambda j, place: (j, 0, 0)),
        ),
        out_shape=jax.ShapeDtypeStruct((count, rows, sum(widths)), jnp.float32),
        compiler_params=pltpu.CompilerParams(vmem_limit_bytes=KERNEL_VMEM),
        name="packed",
    )(place, *[arrays[i] for _, i in parts])


def exchange(place, arrays, first, count, fold):
    sources = arrays[0].shape[2]
    whole = 2 * sources + arrays[2].shape[2]
    up = packed(place, arrays, first, count, fold, ((1, 0), (1, 1), (1, 2), (2, 0), (2, 2)))
    up = shift(up, "y", 1)
    down = packed(place, arrays, first, count, fold, ((3, 0), (3, 1), (3, 2), (2, 1)))
    down = shift(down, "y", -1)
    own = packed(place, arrays, first, count, fold, ((0, 0), (0, 1), (0, 2)))
    far_real, far_imag = shift(up[:, :, whole:], "y", 1), shift(down[:, :, whole:], "y", -1)
    return Share(count, sources, own, up, down, far_real, far_imag)


def on_device(response_real, response_imaginary, focus, initial, onset):
    values = focus.transpose(1, 0, 2)
    local, receivers, width = values.shape
    size, fold, groups = lax.axis_size("z"), lax.axis_size("y"), lax.axis_size("freq")
    freqs = groups * local
    pairs = local // fold
    used = receivers // TILE
    y = lax.axis_index("y")
    place = jnp.stack([lax.axis_index("z"), y]).astype(jnp.int32)
    rows = lax.dynamic_slice_in_dim(onset, lax.axis_index("freq") * TILE, TILE, 0)
    rows = jnp.concatenate([rows, rows], axis=1)
    own = [
        group * local + fold * j + side for side in range(fold) for group in range(groups) for j in range(pairs)
    ]

    def turn(x):
        return lax.all_to_all(x, ("y", "freq"), split_axis=0, concat_axis=0, tiled=True)

    def windowed_rows(x, given):
        x = turn(x).reshape(freqs, TILE, width)
        return window(x, rows, freqs, own, given)

    shares, first = [], 0
    for count in CHUNKS:
        arrays = (response_real, response_imaginary, values)
        shares.append(exchange(place, arrays, first, count, fold))
        first += fold * count

    sums = []
    for share in shares:
        blocks = adjoint_blocks(place, share, width, size)
        sums.append(ring_sum(blocks, "z"))
    adjoint = jnp.concatenate(sums, axis=1).reshape(fold, used, pairs, TILE, width)
    adjoint = jnp.pad(adjoint, ((0, 0), (0, groups - used), (0, 0), (0, 0), (0, 0)))
    windowed = windowed_rows(adjoint.reshape(fold * groups, pairs, TILE, width), own)
    windowed = turn(windowed.reshape(fold * groups, pairs, TILE, width))
    windowed = windowed.reshape(fold, groups, pairs, TILE, width)[:, :used]
    windowed = windowed.reshape(fold * used, pairs, TILE, width)
    part = fold * used // 2
    found = ring_share([windowed[:part], windowed[part:]], "z")
    pieces = [(offset, cut * part, x) for offset, cut, x in found]
    parts, done = [], 0
    for share in shares:
        parts.append(forward_blocks(place, share, pieces, done, size, fold, groups))
        done += share.count
    update = windowed_rows(jnp.concatenate(parts, axis=1), list(range(freqs)))
    update = lax.all_to_all(
        update.reshape(groups, local, TILE, width), "freq", split_axis=0, concat_axis=0, tiled=True
    )
    update = update[:used].transpose(1, 0, 2, 3).reshape(local, receivers, width)
    return initial - update.transpose(1, 0, 2)


def solution(mesh):
    finer = Mesh(mesh.devices.reshape(mesh.shape["freq"], 8, 4), ("freq", "z", "y"))
    in_specs = (
        P("freq", REC, None),
        P("freq", REC, None),
        P(REC, "freq", None),
        P(REC, "freq", None),
        P(REC, None),
    )
    out_specs = P(REC, "freq", None)
    return jax.shard_map(on_device, mesh=finer, in_specs=in_specs, out_specs=out_specs, check_vma=False)
```
